256 devices in a mesh: tmpl: 4 (over x), row: 8 (over y, core), col: 8 (over z).
Axes of the slice: x: 4, y: 4, z: 8, core: 2. Of those that a mesh axis runs over, the one named last changes fastest.
Arguments:
- tmpl_act: bfloat16 [4, 4, 512, 64, 2048], P('tmpl', None, 'row', None, 'col'), may hold values from -4 to 4
- tmpl_bins: int32 [4, 4, 512, 2048], P('tmpl', None, 'row', 'col'), may hold values from 0 to 38
- tmpl_mask: int32 [4, 2048], P('tmpl'), may hold values 0 or 1
- tmpl_aatype: int32 [4, 2048], P('tmpl'), may hold values from 0 to 21
- pair_act: bfloat16 [2048, 2048, 128], P(('tmpl', 'row', 'col')), may hold values from -2.5 to 2.5
- labels: int32 [2048, 2048], P(('tmpl', 'row', 'col')), may hold values from 0 to 63
- bin_embed: bfloat16 [39, 64], replicated, may hold values from -4 to 4
- row_embed: bfloat16 [22, 64], replicated, may hold values from -4 to 4
- col_embed: bfloat16 [22, 64], replicated, may hold values from -4 to 4
- mask_embed: float32 [64], replicated, may hold values from -4 to 4
- layer_gain: float32 [2, 64], replicated, may hold values from 0.1 to 1.9
- w_in: bfloat16 [2, 64, 128], replicated, may hold values from -0.75 to 0.75
- w_out: bfloat16 [2, 128, 64], replicated, may hold values from -0.5 to 0.5
- final_gain: float32 [64], replicated, may hold values from 0.1 to 1.9
- w_query: bfloat16 [128, 64], replicated, may hold values from -0.5 to 0.5
- w_keyval: bfloat16 [64, 128], replicated, may hold values from -0.75 to 0.75
- w_output: bfloat16 [64, 128], replicated, may hold values from -0.75 to 0.75
- head_weight: bfloat16 [128, 64], replicated, may hold values from -0.44921875 to 0.44921875
- head_bias: float32 [64], replicated, may hold values from -3 to 3
Outputs:
- mean_loss: float32 [], replicated
- head_grad: float32 [128, 64], replicated
- bias_grad: float32 [64], replicated
- output_grad: float32 [64, 128], replicated
The draws below stay inside these ranges and needn't reach their ends.
All inputs are finite; a program needn't handle non-finite values. No bound on the sum of `tmpl_mask` on one device may be relied on, other than what follows from the above.
Results may differ from the reference program's by a relative error of at most 0.0003.
Values may be sent and summed in bfloat16 or wider, within the bound.
No kernel may reach another device: no remote copies, remote signals or barrier semaphores. Data moves between devices by JAX's collectives and lax.ppermute only.
A program may use at most 128 MiB of HBM per device.

```python
import math
import jax
import jax.numpy as jnp
from jax import lax

S = 4
C = 64
CZ = 128
HEADS = 4
HEAD_DIM = 16
HIDDEN_SIZE = 128
NBIN = 39
NAA = 22
NB = 64
TLAYERS = 2
N = 2048
GROUPS = 4
HD = 64


def with_ends(array, stream_key, least, largest):
    longest = array.shape.index(max(array.shape))
    spots = []
    for shift in (0, 1):
        where = [jax.random.randint(jax.random.fold_in(stream_key, axis), (), 0, length) for axis, length in enumerate(array.shape)]
        where[longest] = (where[longest] + shift) % array.shape[longest]
        spots.append(tuple(where))
    return array.at[spots[0]].set(least).at[spots[1]].set(largest)


def steps_of(key, dims, cuts, least, high):
    factor_of = 1.0
    for dim, blocks in cuts:
        draws = jax.random.uniform(jax.random.fold_in(jax.random.fold_in(key, 6), dim), (blocks,), jnp.float32, least / len(cuts), high / len(cuts))
        factor_of = factor_of * jnp.repeat(jnp.exp(draws), dims[dim] // blocks).reshape((-1,) + (1,) * (len(dims) - 1 - dim))
    return factor_of


def normal_values(own_key, extent, width, limit, cuts=(), kind=jnp.bfloat16):
    loudness = steps_of(own_key, extent, cuts, -0.22, 0.18) if cuts else 1.0
    drawn = jax.random.normal(own_key, extent, jnp.float32) * width * loudness
    return jnp.minimum(jnp.maximum(drawn, -limit), limit).astype(kind)


def setup_inputs(seed: int = 0) -> dict:
    streams_of = jax.random.split(jax.random.key(seed), 20)
    tmpl_act = normal_values(streams_of[0], (S, GROUPS, N // GROUPS, C, N), 1.0, 4.0, ((0, 4), (2, 8), (4, 8)))
    tmpl_bins = with_ends(jax.random.randint(streams_of[1], (S, GROUPS, N // GROUPS, N), 0, NBIN), jax.random.fold_in(streams_of[1], 1), 0, NBIN - 1).astype(jnp.int32)
    tmpl_mask = with_ends((jax.random.randint(streams_of[2], (S, N), 0, 5) < 4).astype(jnp.int32), jax.random.fold_in(streams_of[2], 1), 0, 1)
    tmpl_aatype = with_ends(jax.random.randint(streams_of[3], (S, N), 0, NAA), jax.random.fold_in(streams_of[3], 1), 0, NAA - 1).astype(jnp.int32)
    pair_act = normal_values(streams_of[4], (N, N, CZ), 1.0, 2.5, ((0, 256),))
    labels = with_ends(jax.random.randint(streams_of[5], (N, N), 0, NB), jax.random.fold_in(streams_of[5], 1), 0, NB - 1).astype(jnp.int32)
    bin_embed = normal_values(streams_of[6], (NBIN, C), 1.0, 4.0)
    row_embed = normal_values(streams_of[7], (NAA, C), 1.0, 4.0)
    col_embed = normal_values(streams_of[8], (NAA, C), 1.0, 4.0)
    mask_embed = normal_values(streams_of[9], (C,), 1.0, 4.0, (), jnp.float32)
    layer_gain = jnp.clip(1.0 + 0.18 * jax.random.normal(streams_of[10], (TLAYERS, C), jnp.float32), 0.1, 1.9)
    w_in = normal_values(streams_of[11], (TLAYERS, C, HIDDEN_SIZE), C ** -0.5, 0.75)
    w_out = normal_values(streams_of[12], (TLAYERS, HIDDEN_SIZE, C), HIDDEN_SIZE ** -0.5, 0.5)
    final_gain = jnp.clip(1.0 + 0.18 * jax.random.normal(streams_of[13], (C,), jnp.float32), 0.1, 1.9)
    w_query = normal_values(streams_of[14], (CZ, HD), CZ ** -0.5, 0.5)
    w_keyval = normal_values(streams_of[15], (C, 2 * HD), C ** -0.5, 0.75)
    w_output = normal_values(streams_of[16], (HD, CZ), HD ** -0.5, 0.75)
    head_weight = jnp.clip(jax.random.uniform(streams_of[17], (CZ, NB), jnp.float32, -0.44921875, 0.44921875), -0.44921875, 0.44921875).astype(jnp.bfloat16)
    head_bias = normal_values(streams_of[18], (NB,), 1.0, 3.0, (), jnp.float32)
    return {"tmpl_act": tmpl_act, "tmpl_bins": tmpl_bins, "tmpl_mask": tmpl_mask, "tmpl_aatype": tmpl_aatype, "pair_act": pair_act, "labels": labels, "bin_embed": bin_embed, "row_embed": row_embed, "col_embed": col_embed, "mask_embed": mask_embed, "layer_gain": layer_gain, "w_in": w_in, "w_out": w_out, "final_gain": final_gain, "w_query": w_query, "w_keyval": w_keyval, "w_output": w_output, "head_weight": head_weight, "head_bias": head_bias}


CLIP_NORM = 16.0

def layer_norm(inputs, gain_vector, channel_axis):
    average = lax.optimization_barrier(jnp.mean(inputs, axis=channel_axis, keepdims=True))
    centered = inputs - average
    spread = lax.optimization_barrier(jnp.mean(centered * centered, axis=channel_axis, keepdims=True))
    return centered * lax.rsqrt(spread + 1e-05) * gain_vector

def reference(tmpl_act, tmpl_bins, tmpl_mask, tmpl_aatype, pair_act, labels, bin_embed, row_embed, col_embed, mask_embed, layer_gain, w_in, w_out, final_gain, w_query, w_keyval, w_output, head_weight, head_bias):
    row_block = 64
    head_width = HEADS * HEAD_DIM
    activations = tmpl_act.reshape(S, N, C, N)
    bin_codes = tmpl_bins.reshape(S, N, N)
    mask_table = tmpl_mask.astype(jnp.float32)
    bin_table = bin_embed.astype(jnp.float32)
    row_table = row_embed.astype(jnp.float32)
    col_terms = col_embed.astype(jnp.float32)[tmpl_aatype]
    levels = jnp.arange(NBIN, dtype=jnp.int32)
    classes = jnp.arange(NB, dtype=jnp.int32)
    w_query32 = w_query.astype(jnp.float32)
    w_keyval32 = w_keyval.astype(jnp.float32)
    w_output32 = w_output.astype(jnp.float32)
    head32 = head_weight.astype(jnp.float32)

    def one_block(offset):
        features = []
        for template in range(S):
            previous = lax.dynamic_slice_in_dim(activations[template], offset, row_block, 0).astype(jnp.float32)
            previous = jnp.swapaxes(previous, 1, 2)
            codes = lax.dynamic_slice_in_dim(bin_codes[template], offset, row_block, 0)
            onehot = (codes[:, :, None] == levels).astype(jnp.float32)
            bin_term = jnp.einsum('ijb,bc->ijc', onehot, bin_table)
            row_mask = lax.dynamic_slice_in_dim(mask_table[template], offset, row_block, 0)
            row_types = lax.dynamic_slice_in_dim(tmpl_aatype[template], offset, row_block, 0)
            pair_mask = row_mask[:, None] * mask_table[template][None, :]
            tmpl_state = previous + pair_mask[:, :, None] * (bin_term + mask_embed) + row_table[row_types][:, None, :] + col_terms[template][None, :, :]
            for layer_index in range(TLAYERS):
                normed = layer_norm(tmpl_state, layer_gain[layer_index], -1).astype(jnp.bfloat16)
                hidden = jax.nn.relu(jnp.einsum('ijc,ce->ije', normed.astype(jnp.float32), w_in[layer_index].astype(jnp.float32))).astype(jnp.bfloat16)
                tmpl_state = tmpl_state + jnp.einsum('ije,ec->ijc', hidden.astype(jnp.float32), w_out[layer_index].astype(jnp.float32))
            features.append(layer_norm(tmpl_state, final_gain, -1).astype(jnp.bfloat16))
        features = jnp.stack(features).astype(jnp.float32)
        pair_rows = lax.dynamic_slice_in_dim(pair_act, offset, row_block, 0).astype(jnp.float32)
        queries = jnp.einsum('ijz,zk->ijk', pair_rows, w_query32).astype(jnp.bfloat16).astype(jnp.float32)
        queries = queries.reshape(row_block, N, HEADS, HEAD_DIM)
        keyval = jnp.einsum('sijc,ck->sijk', features, w_keyval32).astype(jnp.bfloat16).astype(jnp.float32)
        key_heads = keyval[..., :head_width].reshape(S, row_block, N, HEADS, HEAD_DIM)
        value_heads = keyval[..., head_width:].reshape(S, row_block, N, HEADS, HEAD_DIM)
        scores = jnp.einsum('ijhd,sijhd->sijh', queries, key_heads) / math.sqrt(HEAD_DIM)
        exp_scores = jnp.exp(scores)
        weights = (exp_scores / lax.optimization_barrier(jnp.sum(exp_scores, axis=0, keepdims=True))).astype(jnp.bfloat16).astype(jnp.float32)
        mixture = jnp.einsum('sijh,sijhd->ijhd', weights, value_heads).astype(jnp.bfloat16).astype(jnp.float32)
        mixture = mixture.reshape(row_block, N, head_width)
        new_pair = (pair_rows + jnp.einsum('ijk,kz->ijz', mixture, w_output32)).astype(jnp.bfloat16).astype(jnp.float32)
        logits = jnp.einsum('ijz,zb->ijb', new_pair, head32) + head_bias
        exp_logits = jnp.exp(logits)
        partition = lax.optimization_barrier(jnp.sum(exp_logits, axis=-1, keepdims=True))
        label_rows = lax.dynamic_slice_in_dim(labels, offset, row_block, 0)
        target = (label_rows[:, :, None] == classes).astype(jnp.float32)
        cross_entropy = jnp.log(partition[..., 0]) - lax.optimization_barrier(jnp.sum(target * logits, axis=-1))
        logit_grad = ((exp_logits / partition - target) / N).astype(jnp.bfloat16).astype(jnp.float32)
        head_part = jnp.einsum('ijz,ijb->zb', new_pair, logit_grad)
        bias_part = lax.optimization_barrier(jnp.sum(logit_grad, axis=(0, 1)))
        pair_grad = jnp.einsum('ijb,zb->ijz', logit_grad, head32).astype(jnp.bfloat16).astype(jnp.float32)
        output_part = jnp.einsum('ijk,ijz->kz', mixture, pair_grad)
        return (jnp.sum(cross_entropy), head_part, bias_part, output_part)
    offsets = jnp.arange(N // row_block, dtype=jnp.int32) * row_block
    losses, head_parts, bias_parts, output_parts = lax.map(one_block, offsets)
    loss_sum = jnp.sum(losses)
    head_sum = lax.optimization_barrier(jnp.sum(head_parts, axis=0))
    bias_sum = lax.optimization_barrier(jnp.sum(bias_parts, axis=0))
    output_sum = lax.optimization_barrier(jnp.sum(output_parts, axis=0))
    squares = jnp.sum(head_sum * head_sum) + jnp.sum(bias_sum * bias_sum) + jnp.sum(output_sum * output_sum)
    factor = CLIP_NORM / jnp.maximum(jnp.sqrt(squares), CLIP_NORM)
    return (loss_sum / float(N * N), head_sum * factor, bias_sum * factor, output_sum * factor)
```

```python
import functools
import math

import jax
import jax.numpy as jnp
from jax import lax
from jax.experimental import pallas as pl
from jax.experimental.pallas import tpu as pltpu
from jax.sharding import PartitionSpec as P

TMPL_ROW_COL = ("tmpl", "row", "col")
HEADS = 4
HEAD_DIM = 16
CLIP_NORM = 16.0
ROWS = 4
MEMBERS = 2

BIN_ROWS = 48
TYPE_ROWS = 32
MASK_ROW = 40
NO_BIN = 99.0


def norm(state, gain):
    centered = state - jnp.mean(state, axis=0, keepdims=True)
    spread = jnp.mean(centered * centered, axis=0, keepdims=True)
    return (centered * lax.rsqrt(spread + 1e-05) * gain).astype(jnp.bfloat16)


def dot(a, b):
    return lax.dot_general(a, b, (((1,), (0,)), ((), ())), preferred_element_type=jnp.float32)


def dot_t(a, b):
    return lax.dot_general(a, b, (((1,), (1,)), ((), ())), preferred_element_type=jnp.float32)


def chunk_kernel(
    count,
    rows,
    residues,
    where_ref,
    types_ref,
    *refs,
):
    own_ref, *act_refs = refs[:4]
    pair_refs = refs[4 : 4 + count]
    label_refs = refs[4 + count : 4 + 2 * count]
    (
        code_ref, col_ref, table_ref, gain_ref, w_in_ref, w_out_ref, w_kv_ref, w_qp_ref,
        w_o_ref, head_ref, bias_ref, acc_in_ref, loss_in_ref, acc_ref, loss_ref, label_scratch,
    ) = refs[4 + 2 * count :]
    step = pl.program_id(0)
    steps = pl.num_programs(0) // count
    channels, width = own_ref.shape[-2:]
    templates = 4
    lanes = label_scratch.shape[-1]
    pieces = width // lanes
    within = lax.rem(step, steps)
    base = within * rows

    @pl.when(step == 0)
    def _():
        acc_ref[...] = acc_in_ref[...]
        loss_ref[...] = loss_in_ref[...]
        for k in range(count):
            label_scratch[k] = label_refs[k][...].astype(jnp.float32)

    member = step // steps
    residue = where_ref[2 + member] * 8 + base
    bin_index = lax.broadcasted_iota(jnp.int32, (BIN_ROWS, width), 0).astype(jnp.float32)
    type_index = lax.broadcasted_iota(jnp.int32, (TYPE_ROWS, width), 0)
    class_index = lax.broadcasted_iota(jnp.int32, (head_ref.shape[0], width), 0).astype(
        jnp.float32
    )
    mask_rows = bin_index >= float(MASK_ROW)

    operand, previous = [], []
    for row in range(rows):
        for s in range(templates):
            code = code_ref[s, pl.ds(base + row, 1), :]
            present = jnp.where(code < NO_BIN, 1.0, 0.0)
            hot = jnp.where(mask_rows, present, jnp.where(bin_index == code, 1.0, 0.0))
            kind = types_ref[s, residue + row]
            row_hot = jnp.where(type_index == kind, 1.0, 0.0)
            operand.append(
                jnp.concatenate(
                    [hot.astype(jnp.bfloat16), row_hot.astype(jnp.bfloat16), col_ref[s]], axis=0
                )
            )
            act = own_ref[0, row] if s == 0 else act_refs[s - 1][row]
            previous.append(act.astype(jnp.float32))
    state = jnp.concatenate(previous, axis=1) + dot(
        table_ref[...], jnp.concatenate(operand, axis=1)
    )
    for layer in range(w_in_ref.shape[0]):
        normed = norm(state, gain_ref[:, layer : layer + 1])
        hidden = jnp.maximum(dot(w_in_ref[layer], normed).astype(jnp.bfloat16), 0.0)
        state = state + dot(w_out_ref[layer], hidden)
    features = norm(state, gain_ref[:, w_in_ref.shape[0] : w_in_ref.shape[0] + 1])
    keyval = dot(w_kv_ref[...], features).astype(jnp.bfloat16)

    head_width = HEADS * HEAD_DIM
    for row in range(rows):
        pairs = [
            ref[row] if len(ref.shape) == 3 else ref[row * width : (row + 1) * width, :]
            for ref in pair_refs
        ]
        pair = pairs[0]
        for k in range(1, count):
            pair = jnp.where(member == k, pairs[k], pair)
        label = jnp.concatenate(
            [
                label_scratch[member, pl.ds((base + row) * pieces + k, 1), :]
                for k in range(pieces)
            ],
            axis=1,
        )
        projected = dot_t(w_qp_ref[...], pair)
        queries = projected[:head_width].astype(jnp.bfloat16).astype(jnp.float32)
        pair_rows = projected[head_width:]
        exps, values = [], []
        for s in range(templates):
            at = (row * templates + s) * width
            keys = keyval[:head_width, at : at + width].astype(jnp.float32)
            values.append(keyval[head_width:, at : at + width].astype(jnp.float32))
            scores = jnp.sum(
                (queries * keys).reshape(HEADS, HEAD_DIM, width), axis=1, keepdims=True
            ) * (1.0 / math.sqrt(HEAD_DIM))
            exps.append(jnp.exp(scores))
        total = exps[0] + exps[1] + exps[2] + exps[3]
        mixture = None
        for s in range(templates):
            weight = (exps[s] / total).astype(jnp.bfloat16).astype(jnp.float32)
            term = weight * values[s].reshape(HEADS, HEAD_DIM, width)
            mixture = term if mixture is None else mixture + term
        mixture = mixture.reshape(head_width, width).astype(jnp.bfloat16)
        new_pair = (pair_rows + dot(w_o_ref[...], mixture)).astype(jnp.bfloat16)
        logits = dot(head_ref[...], new_pair) + bias_ref[...]
        exp_logits = jnp.exp(logits)
        partition = jnp.sum(exp_logits, axis=0, keepdims=True)
        target = class_index == label
        picked = jnp.sum(jnp.where(target, logits, 0.0), axis=0, keepdims=True)
        loss_ref[0:1, :] += jnp.log(partition) - picked
        grad = (
            (exp_logits / partition - jnp.where(target, 1.0, 0.0)) * (1.0 / residues)
        ).astype(jnp.bfloat16)
        left = jnp.concatenate(
            [new_pair, mixture, jnp.ones((16, width), jnp.bfloat16)], axis=0
        )
        acc_ref[...] += dot_t(left, grad)


def run_chunk(residues, where, types, own, acts, pairs, labels, code, col_hot, weights, acc, loss):
    count = len(pairs)
    channels, width = own.shape[2:]
    pair_width = pairs[0].shape[-1]
    steps = 8 // ROWS
    lanes = labels[0].shape[-1]
    label_rows = 8 * width // lanes

    def whole(array):
        zeros = (0,) * array.ndim
        return pl.BlockSpec(array.shape, lambda i, *_: zeros, pipeline_mode=pl.Buffered(1))

    def pair_spec(k, array):
        def at(i):
            return jnp.clip(i - k * steps, 0, steps - 1)

        if array.ndim == 3:
            return pl.BlockSpec((ROWS, width, pair_width), lambda i, w, t: (at(i), w[1], 0))
        return pl.BlockSpec((ROWS * width, pair_width), lambda i, w, t: (at(i), 0))

    def label_spec(array):
        last = array.shape[0] // label_rows - 1
        return pl.BlockSpec(
            (label_rows, lanes), lambda i, *_: (last, 0), pipeline_mode=pl.Buffered(1)
        )

    in_specs = (
        [
            pl.BlockSpec(
                (1, ROWS, channels, width),
                lambda i, w, t: (w[0], w[2 + i // steps] * steps + lax.rem(i, steps), 0, 0),
            )
        ]
        + [
            pl.BlockSpec(
                (ROWS, channels, width),
                lambda i, w, t: (
                    lax.rem(w[2 + i // steps], MEMBERS) * steps + lax.rem(i, steps), 0, 0
                ),
            )
        ]
        * 3
        + [pair_spec(k, array) for k, array in enumerate(pairs)]
        + [label_spec(array) for array in labels]
        + [pl.BlockSpec((4, 8, width), lambda i, w, t: (0, w[2 + i // steps], 0))]
        + [whole(w) for w in (col_hot, *weights, acc, loss)]
    )
    return pl.pallas_call(
        functools.partial(chunk_kernel, count, ROWS, residues),
        out_shape=(
            jax.ShapeDtypeStruct(acc.shape, jnp.float32),
            jax.ShapeDtypeStruct(loss.shape, jnp.float32),
        ),
        grid_spec=pltpu.PrefetchScalarGridSpec(
            num_scalar_prefetch=2,
            grid=(count * steps,),
            in_specs=in_specs,
            out_specs=(
                pl.BlockSpec(acc.shape, lambda i, *_: (0, 0)),
                pl.BlockSpec(loss.shape, lambda i, *_: (0, 0)),
            ),
            scratch_shapes=[pltpu.VMEM((count, label_rows, lanes), jnp.float32)],
        ),
        compiler_params=pltpu.CompilerParams(
            dimension_semantics=("arbitrary",), vmem_limit_bytes=48 << 20
        ),
        cost_estimate=pl.CostEstimate(
            flops=count * 3_000_000_000, transcendentals=0, bytes_accessed=count << 20
        ),
        name="fused_rows",
    )(where, types, own, *acts, *pairs, *labels, code, col_hot, *weights, acc, loss)


def pack_kernel(plan, where_ref, act_ref, pair_ref, codes_ref, labels_ref, *refs):
    outs, next_ref = refs[: len(plan)], refs[len(plan)]
    in_sems, out_sems = refs[len(plan) + 1 : len(plan) + 3]
    buffers = refs[len(plan) + 3 :]
    x, z = where_ref[0], where_ref[1]
    next_ref[0] = x
    next_ref[1] = z
    rows, width = pair_ref.shape[0], codes_ref.shape[-1]
    pairs = []
    for (kind, value, first), out, buffer in zip(plan, outs, buffers):
        if kind == "group":
            other = lax.rem(x + value, act_ref.shape[0])
            start = pl.multiple_of(first_member(z, first) * rows, MEMBERS * rows)
            at = MEMBERS * rows
            pairs.append((act_ref.at[other, pl.ds(start, at)], buffer.at[:at], out.at[:at]))
            if first == 0:
                bins = act_ref.shape[2]
                planes = codes_ref.shape[1] - bins
                tables = (at + 1, slice(0, planes))
                pairs.append((codes_ref.at[other, :bins], buffer.at[at], out.at[at]))
                pairs.append((codes_ref.at[other, bins:], buffer.at[tables], out.at[tables]))
        else:
            other = z ^ value
            start = pl.multiple_of(other * width, width)
            for row in range(rows):
                block = slice(row * width, (row + 1) * width)
                pairs.append((pair_ref.at[row, pl.ds(start, width)], buffer.at[block], out.at[block]))
            tail = slice(rows * width, None)
            pairs.append((labels_ref.at[other], buffer.at[tail], out.at[tail]))
    loads = [
        pltpu.make_async_copy(source, buffer, in_sems.at[k])
        for k, (source, buffer, _) in enumerate(pairs)
    ]
    stores = [
        pltpu.make_async_copy(buffer, target, out_sems.at[k])
        for k, (_, buffer, target) in enumerate(pairs)
    ]
    for load in loads:
        load.start()
    for load, store in zip(loads, stores):
        load.wait()
        store.start()
    for store in stores:
        store.wait()


def first_member(z, first):
    both = z ^ first
    return both - lax.rem(both, MEMBERS)


def pack(plan, where, act, pair, codes, labels):
    rows, width = pair.shape[0], codes.shape[-1]
    shapes = []
    count = 0
    for kind, _, first in plan:
        if kind == "group":
            extra = 2 if first == 0 else 0
            shapes.append((MEMBERS * rows + extra,) + act.shape[2:])
            count += 1 + extra
        else:
            shapes.append((rows * width + labels.shape[1], pair.shape[2]))
            count += rows + 1
    hbm = pl.BlockSpec(memory_space=pltpu.MemorySpace.HBM)
    return pl.pallas_call(
        functools.partial(pack_kernel, plan),
        out_shape=[jax.ShapeDtypeStruct(shape, jnp.bfloat16) for shape in shapes]
        + [jax.ShapeDtypeStruct(where.shape, where.dtype)],
        in_specs=[pl.BlockSpec(memory_space=pltpu.MemorySpace.SMEM)] + [hbm] * 4,
        out_specs=[hbm] * len(plan) + [pl.BlockSpec(memory_space=pltpu.MemorySpace.SMEM)],
        scratch_shapes=[pltpu.SemaphoreType.DMA((count,))] * 2
        + [pltpu.VMEM(shape, jnp.bfloat16) for shape in shapes],
        name="pack",
    )(where, act, pair, codes, labels)


def transpose_bf16(array):
    return jnp.swapaxes(array, -1, -2)


def prepare_weights(
    bin_embed, row_embed, col_embed, mask_embed, layer_gain, w_in, w_out, final_gain,
    w_query, w_keyval, w_output, head_weight, head_bias,
):
    channels = bin_embed.shape[1]
    pair_width = w_query.shape[0]
    part0 = lax.reduce_precision(mask_embed, 8, 7)
    rest = mask_embed - part0
    part1 = lax.reduce_precision(rest, 8, 7)
    part2 = rest - part1
    parts = jnp.stack([part0, part1, part2]).astype(jnp.bfloat16)

    def padded(array, rows):
        return jnp.pad(array, ((0, rows - array.shape[0]), (0, 0)))

    table = jnp.concatenate(
        [
            padded(bin_embed, MASK_ROW),
            padded(parts, BIN_ROWS - MASK_ROW),
            padded(row_embed, TYPE_ROWS),
            padded(col_embed, TYPE_ROWS),
        ]
    ).T
    gains = jnp.concatenate([layer_gain, final_gain[None]]).T
    w_qp = jnp.concatenate([w_query.T, jnp.eye(pair_width, dtype=jnp.bfloat16)])
    return (
        table,
        gains,
        transpose_bf16(w_in),
        transpose_bf16(w_out),
        w_keyval.T,
        w_qp,
        w_output.T,
        head_weight.T,
        head_bias[:, None],
    )


def total_over_mesh(part):
    def gathered(part, axis_name, links):
        others = [lax.ppermute(part, axis_name, pairs) for pairs in links]
        for other in others:
            part = part + other
        return part

    groups, rows, cols = (lax.axis_size(name) for name in TMPL_ROW_COL)
    part = gathered(part, "row", [[(i, i ^ 1) for i in range(rows)]])
    part = gathered(
        part, "tmpl", [[(i, (i + e) % groups) for i in range(groups)] for e in range(1, groups)]
    )
    part = gathered(
        part, "row", [[(i, (i + e) % rows) for i in range(rows)] for e in range(2, rows, 2)]
    )
    bit = 1
    while bit < cols:
        part = gathered(part, "col", [[(i, i ^ bit) for i in range(cols)]])
        bit *= 2
    return part


def on_device(
    tmpl_act, tmpl_bins, tmpl_mask, tmpl_aatype, pair_act, labels, bin_embed, row_embed,
    col_embed, mask_embed, layer_gain, w_in, w_out, final_gain, w_query, w_keyval,
    w_output, head_weight, head_bias,
):
    groups = lax.axis_size("tmpl")
    cols = lax.axis_size("col")
    residues = tmpl_mask.shape[1]
    group_rows = tmpl_bins.shape[2]
    width = tmpl_bins.shape[3]
    rows = group_rows // cols
    channels = tmpl_act.shape[3]
    pair_width = pair_act.shape[2]
    x, z = lax.axis_index("tmpl"), lax.axis_index("col")
    row_offset = lax.axis_index("row") * group_rows
    act = tmpl_act[0]

    tables = jnp.concatenate([tmpl_mask, tmpl_aatype]).reshape(1, -1, width)
    tables = jnp.broadcast_to(tables, (groups,) + tables.shape[1:])
    codes = jnp.concatenate([tmpl_bins[0], tables], axis=1).astype(jnp.bfloat16)
    lanes = pair_width
    label_blocks = labels.reshape(rows, cols, width).astype(jnp.bfloat16)
    label_blocks = jnp.swapaxes(label_blocks, 0, 1).reshape(cols, -1, lanes)

    place = jnp.stack([x, z]).astype(jnp.int32)
    order = (1, 3, 2)
    moved = {}
    for first in range(0, cols, MEMBERS):
        plan = [("group", e, first) for e in order]
        plan += [("column", d, 0) for d in range(max(first, 1), first + MEMBERS)]
        *messages, place = pack(tuple(plan), place, act, pair_act, codes, label_blocks)
        for (kind, value, first), message in zip(plan, messages):
            if kind == "group":
                links = [(i, (i + value) % groups) for i in range(groups)]
                moved[kind, value, first] = lax.ppermute(message, "tmpl", links)
            else:
                links = [(i, i ^ value) for i in range(cols)]
                moved[kind, value, first] = lax.ppermute(message, "col", links)

    weights = prepare_weights(
        bin_embed, row_embed, col_embed, mask_embed, layer_gain, w_in, w_out, final_gain,
        w_query, w_keyval, w_output, head_weight, head_bias,
    )
    own_codes = lax.dynamic_index_in_dim(codes, x, 0, False)
    first_messages = [moved["group", e, 0] for e in order]
    bins = jnp.stack([own_codes[:group_rows]] + [m[-2] for m in first_messages])
    tables = jnp.stack(
        [own_codes[group_rows:]] + [m[-1, : codes.shape[1] - group_rows] for m in first_messages]
    )
    tables = tables.astype(jnp.float32).reshape(groups, 2, residues)
    here = lax.dynamic_slice_in_dim(tables, z * width, width, 2)
    group_offset = x * (residues // groups) + row_offset
    there = lax.dynamic_slice_in_dim(tables, group_offset, group_rows, 2)
    masked = there[:, 0, :, None] * here[:, 0, None, :]
    bins = jnp.where(masked > 0.5, bins.astype(jnp.float32), NO_BIN)
    row_types = there[:, 1].astype(jnp.int32)
    kinds = jnp.arange(TYPE_ROWS, dtype=jnp.float32)
    col_hot = (here[:, 1, None, :] == kinds[None, :, None]).astype(jnp.bfloat16)
    own_labels = lax.dynamic_index_in_dim(label_blocks, z, 0, False)

    acc = jnp.zeros((pair_width + HEADS * HEAD_DIM + 16, head_weight.shape[1]), jnp.float32)
    loss = jnp.zeros((8, width), jnp.float32)
    for first in range(0, cols, MEMBERS):
        members = range(first, first + MEMBERS)
        where = jnp.stack([x, z] + [z ^ d for d in members]).astype(jnp.int32)
        acc, loss = run_chunk(
            residues, where, row_types, act, [moved["group", e, first] for e in order],
            [moved["column", d, 0] if d else pair_act for d in members],
            [moved["column", d, 0] if d else own_labels for d in members],
            bins, col_hot, weights, acc, loss,
        )

    half, classes = acc.shape[0] // 2, acc.shape[1]
    head_width = HEADS * HEAD_DIM
    bias_row = pair_width + head_width
    sums = jnp.concatenate([acc[:half], acc[half:]], axis=1)
    at_loss = (jnp.arange(half)[:, None] == bias_row + 1 - half) & (
        jnp.arange(2 * classes)[None, :] >= classes
    )
    sums = total_over_mesh(jnp.where(at_loss, jnp.sum(loss), sums))
    sums = jnp.concatenate([sums[:, :classes], sums[:, classes:]])
    head_sum = sums[:pair_width]
    bias_sum = sums[bias_row]
    output_sum = lax.dot_general(
        sums[pair_width:bias_row],
        head_weight.astype(jnp.float32),
        (((1,), (1,)), ((), ())),
        precision=lax.Precision.HIGHEST,
    )
    squares = (
        jnp.sum(head_sum * head_sum)
        + jnp.sum(bias_sum * bias_sum)
        + jnp.sum(output_sum * output_sum)
    )
    factor = CLIP_NORM / jnp.maximum(jnp.sqrt(squares), CLIP_NORM)
    return (
        sums[bias_row + 1, 0] / float(residues * residues),
        head_sum * factor,
        bias_sum * factor,
        output_sum * factor,
    )


def solution(mesh):
    in_specs = (
        P("tmpl", None, "row", None, "col"),
        P("tmpl", None, "row", "col"),
        P("tmpl", None),
        P("tmpl", None),
        P(TMPL_ROW_COL, None, None),
        P(TMPL_ROW_COL, None),
    ) + (P(),) * 13
    return jax.shard_map(
        on_device, mesh=mesh, in_specs=in_specs, out_specs=(P(),) * 4, check_vma=False
    )
```

```python
import functools
import math

import jax
import jax.numpy as jnp
from jax import lax
from jax.experimental import pallas as pl
from jax.experimental.pallas import tpu as pltpu
from jax.sharding import PartitionSpec as P

TMPL_ROW_COL = ("tmpl", "row", "col")
HEADS = 4
HEAD_DIM = 16
CLIP_NORM = 16.0
ROWS = 4
MEMBERS = 2
AHEAD = 3

BIN_ROWS = 48
TYPE_ROWS = 32
MASK_ROW = 40
NO_BIN = 99.0


def norm(state, gain):
    centered = state - jnp.mean(state, axis=0, keepdims=True)
    spread = jnp.mean(centered * centered, axis=0, keepdims=True)
    return (centered * lax.rsqrt(spread + 1e-05) * gain).astype(jnp.bfloat16)


def dot(a, b):
    return lax.dot_general(a, b, (((1,), (0,)), ((), ())), preferred_element_type=jnp.float32)


def dot_t(a, b):
    return lax.dot_general(a, b, (((1,), (1,)), ((), ())), preferred_element_type=jnp.float32)


def chunk_kernel(
    count,
    rows,
    residues,
    where_ref,
    types_ref,
    *refs,
):
    own_ref, *act_refs = refs[:4]
    pair_refs = refs[4 : 4 + count]
    label_refs = refs[4 + count : 4 + 2 * count]
    (
        code_ref, col_ref, table_ref, gain_ref, w_in_ref, w_out_ref, w_kv_ref, w_qp_ref,
        w_o_ref, head_ref, bias_ref, acc_in_ref, loss_in_ref, acc_ref, loss_ref, token_ref, label_scratch,
    ) = refs[4 + 2 * count :]
    step = pl.program_id(0)
    steps = pl.num_programs(0) // count
    channels, width = own_ref.shape[-2:]
    templates = 4
    lanes = label_scratch.shape[-1]
    pieces = width // lanes
    within = lax.rem(step, steps)
    base = within * rows

    @pl.when(step == 0)
    def _():
        acc_ref[...] = acc_in_ref[...]
        loss_ref[...] = loss_in_ref[...]
        token_ref[0] = where_ref[0]
        token_ref[1] = where_ref[1]
        for k in range(count):
            label_scratch[k] = label_refs[k][...].astype(jnp.float32)

    member = step // steps
    residue = where_ref[2 + member] * 8 + base
    bin_index = lax.broadcasted_iota(jnp.int32, (BIN_ROWS, width), 0).astype(jnp.float32)
    type_index = lax.broadcasted_iota(jnp.int32, (TYPE_ROWS, width), 0)
    class_index = lax.broadcasted_iota(jnp.int32, (head_ref.shape[0], width), 0).astype(
        jnp.float32
    )
    mask_rows = bin_index >= float(MASK_ROW)

    operand, previous = [], []
    for row in range(rows):
        for s in range(templates):
            code = code_ref[s, pl.ds(base + row, 1), :]
            present = jnp.where(code < NO_BIN, 1.0, 0.0)
            hot = jnp.where(mask_rows, present, jnp.where(bin_index == code, 1.0, 0.0))
            kind = types_ref[s, residue + row]
            row_hot = jnp.where(type_index == kind, 1.0, 0.0)
            operand.append(
                jnp.concatenate(
                    [hot.astype(jnp.bfloat16), row_hot.astype(jnp.bfloat16), col_ref[s]], axis=0
                )
            )
            act = own_ref[0, row] if s == 0 else act_refs[s - 1][row]
            previous.append(act.astype(jnp.float32))
    state = jnp.concatenate(previous, axis=1) + dot(
        table_ref[...], jnp.concatenate(operand, axis=1)
    )
    for layer in range(w_in_ref.shape[0]):
        normed = norm(state, gain_ref[:, layer : layer + 1])
        hidden = jnp.maximum(dot(w_in_ref[layer], normed).astype(jnp.bfloat16), 0.0)
        state = state + dot(w_out_ref[layer], hidden)
    features = norm(state, gain_ref[:, w_in_ref.shape[0] : w_in_ref.shape[0] + 1])
    keyval = dot(w_kv_ref[...], features).astype(jnp.bfloat16)

    head_width = HEADS * HEAD_DIM
    for row in range(rows):
        pairs = [
            ref[row] if len(ref.shape) == 3 else ref[row * width : (row + 1) * width, :]
            for ref in pair_refs
        ]
        pair = pairs[0]
        for k in range(1, count):
            pair = jnp.where(member == k, pairs[k], pair)
        label = jnp.concatenate(
            [
                label_scratch[member, pl.ds((base + row) * pieces + k, 1), :]
                for k in range(pieces)
            ],
            axis=1,
        )
        projected = dot_t(w_qp_ref[...], pair)
        queries = projected[:head_width].astype(jnp.bfloat16).astype(jnp.float32)
        pair_rows = projected[head_width:]
        exps, values = [], []
        for s in range(templates):
            at = (row * templates + s) * width
            keys = keyval[:head_width, at : at + width].astype(jnp.float32)
            values.append(keyval[head_width:, at : at + width].astype(jnp.float32))
            scores = jnp.sum(
                (queries * keys).reshape(HEADS, HEAD_DIM, width), axis=1, keepdims=True
            ) * (1.0 / math.sqrt(HEAD_DIM))
            exps.append(jnp.exp(scores))
        total = exps[0] + exps[1] + exps[2] + exps[3]
        mixture = None
        for s in range(templates):
            weight = (exps[s] / total).astype(jnp.bfloat16).astype(jnp.float32)
            term = weight * values[s].reshape(HEADS, HEAD_DIM, width)
            mixture = term if mixture is None else mixture + term
        mixture = mixture.reshape(head_width, width).astype(jnp.bfloat16)
        new_pair = (pair_rows + dot(w_o_ref[...], mixture)).astype(jnp.bfloat16)
        logits = dot(head_ref[...], new_pair) + bias_ref[...]
        exp_logits = jnp.exp(logits)
        partition = jnp.sum(exp_logits, axis=0, keepdims=True)
        target = class_index == label
        picked = jnp.sum(jnp.where(target, logits, 0.0), axis=0, keepdims=True)
        loss_ref[0:1, :] += jnp.log(partition) - picked
        grad = (
            (exp_logits / partition - jnp.where(target, 1.0, 0.0)) * (1.0 / residues)
        ).astype(jnp.bfloat16)
        left = jnp.concatenate(
            [new_pair, mixture, jnp.ones((16, width), jnp.bfloat16)], axis=0
        )
        acc_ref[...] += dot_t(left, grad)


def run_chunk(residues, where, types, own, acts, pairs, labels, code, col_hot, weights, acc, loss):
    count = len(pairs)
    channels, width = own.shape[2:]
    pair_width = pairs[0].shape[-1]
    steps = 8 // ROWS
    lanes = labels[0].shape[-1]
    label_rows = 8 * width // lanes

    def whole(array):
        zeros = (0,) * array.ndim
        return pl.BlockSpec(array.shape, lambda i, *_: zeros, pipeline_mode=pl.Buffered(1))

    def pair_spec(k, array):
        def at(i):
            return jnp.clip(i - k * steps, 0, steps - 1)

        if array.ndim == 3:
            return pl.BlockSpec((ROWS, width, pair_width), lambda i, w, t: (at(i), w[1], 0))
        return pl.BlockSpec((ROWS * width, pair_width), lambda i, w, t: (at(i), 0))

    def label_spec(array):
        last = array.shape[0] // label_rows - 1
        return pl.BlockSpec(
            (label_rows, lanes), lambda i, *_: (last, 0), pipeline_mode=pl.Buffered(1)
        )

    in_specs = (
        [
            pl.BlockSpec(
                (1, ROWS, channels, width),
                lambda i, w, t: (w[0], w[2 + i // steps] * steps + lax.rem(i, steps), 0, 0),
            )
        ]
        + [
            pl.BlockSpec(
                (ROWS, channels, width),
                lambda i, w, t: (
                    lax.rem(w[2 + i // steps], MEMBERS) * steps + lax.rem(i, steps), 0, 0
                ),
            )
        ]
        * 3
        + [pair_spec(k, array) for k, array in enumerate(pairs)]
        + [label_spec(array) for array in labels]
        + [pl.BlockSpec((4, 8, width), lambda i, w, t: (0, w[2 + i // steps], 0))]
        + [whole(w) for w in (col_hot, *weights, acc, loss)]
    )
    return pl.pallas_call(
        functools.partial(chunk_kernel, count, ROWS, residues),
        out_shape=(
            jax.ShapeDtypeStruct(acc.shape, jnp.float32),
            jax.ShapeDtypeStruct(loss.shape, jnp.float32),
            jax.ShapeDtypeStruct((2,), jnp.int32),
        ),
        grid_spec=pltpu.PrefetchScalarGridSpec(
            num_scalar_prefetch=2,
            grid=(count * steps,),
            in_specs=in_specs,
            out_specs=(
                pl.BlockSpec(acc.shape, lambda i, *_: (0, 0)),
                pl.BlockSpec(loss.shape, lambda i, *_: (0, 0)),
                pl.BlockSpec(memory_space=pltpu.MemorySpace.SMEM),
            ),
            scratch_shapes=[pltpu.VMEM((count, label_rows, lanes), jnp.float32)],
        ),
        compiler_params=pltpu.CompilerParams(
            dimension_semantics=("arbitrary",), vmem_limit_bytes=48 << 20,
        ),
        cost_estimate=pl.CostEstimate(
            flops=count * 3_000_000_000, transcendentals=0, bytes_accessed=count << 20
        ),
        name="fused_rows",
    )(where, types, own, *acts, *pairs, *labels, code, col_hot, *weights, acc, loss)


def pack_kernel(plan, where_ref, act_ref, pair_ref, codes_ref, labels_ref, *refs):
    outs, next_ref = refs[: len(plan)], refs[len(plan)]
    in_sems, out_sems = refs[len(plan) + 1 : len(plan) + 3]
    buffers = refs[len(plan) + 3 :]
    x, z = where_ref[0], where_ref[1]
    next_ref[0] = x
    next_ref[1] = z
    rows, width = pair_ref.shape[0], codes_ref.shape[-1]
    pairs = []
    for (kind, value, first), out, buffer in zip(plan, outs, buffers):
        if kind == "group":
            other = lax.rem(x + value, act_ref.shape[0])
            start = pl.multiple_of(first_member(z, first) * rows, MEMBERS * rows)
            at = MEMBERS * rows
            pairs.append((act_ref.at[other, pl.ds(start, at)], buffer.at[:at], out.at[:at]))
            if first == 0:
                bins = act_ref.shape[2]
                planes = codes_ref.shape[1] - bins
                tables = (at + 1, slice(0, planes))
                pairs.append((codes_ref.at[other, :bins], buffer.at[at], out.at[at]))
                pairs.append((codes_ref.at[other, bins:], buffer.at[tables], out.at[tables]))
        else:
            other = z ^ value
            start = pl.multiple_of(other * width, width)
            for row in range(rows):
                block = slice(row * width, (row + 1) * width)
                pairs.append((pair_ref.at[row, pl.ds(start, width)], buffer.at[block], out.at[block]))
            tail = slice(rows * width, None)
            pairs.append((labels_ref.at[other], buffer.at[tail], out.at[tail]))
    loads = [
        pltpu.make_async_copy(source, buffer, in_sems.at[k])
        for k, (source, buffer, _) in enumerate(pairs)
    ]
    stores = [
        pltpu.make_async_copy(buffer, target, out_sems.at[k])
        for k, (_, buffer, target) in enumerate(pairs)
    ]
    for load in loads:
        load.start()
    for load, store in zip(loads, stores):
        load.wait()
        store.start()
    for store in stores:
        store.wait()


def first_member(z, first):
    both = z ^ first
    return both - lax.rem(both, MEMBERS)


def pack(plan, where, act, pair, codes, labels):
    rows, width = pair.shape[0], codes.shape[-1]
    shapes = []
    count = 0
    for kind, _, first in plan:
        if kind == "group":
            extra = 2 if first == 0 else 0
            shapes.append((MEMBERS * rows + extra,) + act.shape[2:])
            count += 1 + extra
        else:
            shapes.append((rows * width + labels.shape[1], pair.shape[2]))
            count += rows + 1
    hbm = pl.BlockSpec(memory_space=pltpu.MemorySpace.HBM)
    return pl.pallas_call(
        functools.partial(pack_kernel, plan),
        out_shape=[jax.ShapeDtypeStruct(shape, jnp.bfloat16) for shape in shapes]
        + [jax.ShapeDtypeStruct(where.shape, where.dtype)],
        in_specs=[pl.BlockSpec(memory_space=pltpu.MemorySpace.SMEM)] + [hbm] * 4,
        out_specs=[hbm] * len(plan) + [pl.BlockSpec(memory_space=pltpu.MemorySpace.SMEM)],
        scratch_shapes=[pltpu.SemaphoreType.DMA((count,))] * 2
        + [pltpu.VMEM(shape, jnp.bfloat16) for shape in shapes],
        name="pack",
    )(where, act, pair, codes, labels)


def transpose_bf16(array):
    return jnp.swapaxes(array, -1, -2)


def prepare_weights(
    bin_embed, row_embed, col_embed, mask_embed, layer_gain, w_in, w_out, final_gain,
    w_query, w_keyval, w_output, head_weight, head_bias,
):
    channels = bin_embed.shape[1]
    pair_width = w_query.shape[0]
    part0 = lax.reduce_precision(mask_embed, 8, 7)
    rest = mask_embed - part0
    part1 = lax.reduce_precision(rest, 8, 7)
    part2 = rest - part1
    parts = jnp.stack([part0, part1, part2]).astype(jnp.bfloat16)

    def padded(array, rows):
        return jnp.pad(array, ((0, rows - array.shape[0]), (0, 0)))

    table = jnp.concatenate(
        [
            padded(bin_embed, MASK_ROW),
            padded(parts, BIN_ROWS - MASK_ROW),
            padded(row_embed, TYPE_ROWS),
            padded(col_embed, TYPE_ROWS),
        ]
    ).T
    gains = jnp.concatenate([layer_gain, final_gain[None]]).T
    w_qp = jnp.concatenate([w_query.T, jnp.eye(pair_width, dtype=jnp.bfloat16)])
    return (
        table,
        gains,
        transpose_bf16(w_in),
        transpose_bf16(w_out),
        w_keyval.T,
        w_qp,
        w_output.T,
        head_weight.T,
        head_bias[:, None],
    )


def total_over_mesh(part):
    def gathered(part, axis_name, links):
        others = [lax.ppermute(part, axis_name, pairs) for pairs in links]
        for other in others:
            part = part + other
        return part

    groups, rows, cols = (lax.axis_size(name) for name in TMPL_ROW_COL)
    part = gathered(part, "row", [[(i, i ^ 1) for i in range(rows)]])
    part = gathered(
        part, "tmpl", [[(i, (i + e) % groups) for i in range(groups)] for e in range(1, groups)]
    )
    part = gathered(
        part, "row", [[(i, (i + e) % rows) for i in range(rows)] for e in range(2, rows, 2)]
    )
    bit = 1
    while bit < cols:
        part = gathered(part, "col", [[(i, i ^ bit) for i in range(cols)]])
        bit *= 2
    return part


def on_device(
    tmpl_act, tmpl_bins, tmpl_mask, tmpl_aatype, pair_act, labels, bin_embed, row_embed,
    col_embed, mask_embed, layer_gain, w_in, w_out, final_gain, w_query, w_keyval,
    w_output, head_weight, head_bias,
):
    groups = lax.axis_size("tmpl")
    cols = lax.axis_size("col")
    residues = tmpl_mask.shape[1]
    group_rows = tmpl_bins.shape[2]
    width = tmpl_bins.shape[3]
    rows = group_rows // cols
    channels = tmpl_act.shape[3]
    pair_width = pair_act.shape[2]
    x, z = lax.axis_index("tmpl"), lax.axis_index("col")
    row_offset = lax.axis_index("row") * group_rows
    act = tmpl_act[0]

    tables = jnp.concatenate([tmpl_mask, tmpl_aatype]).reshape(1, -1, width)
    tables = jnp.broadcast_to(tables, (groups,) + tables.shape[1:])
    codes = jnp.concatenate([tmpl_bins[0], tables], axis=1).astype(jnp.bfloat16)
    lanes = pair_width
    label_blocks = labels.reshape(rows, cols, width).astype(jnp.bfloat16)
    label_blocks = jnp.swapaxes(label_blocks, 0, 1).reshape(cols, -1, lanes)

    place = jnp.stack([x, z]).astype(jnp.int32)
    order = (1, 3, 2)
    moved = {}

    def send(first, place):
        plan = [("column", d, 0) for d in range(max(first, 1), first + MEMBERS)]
        plan += [("group", e, first) for e in order]
        *messages, place = pack(tuple(plan), place, act, pair_act, codes, label_blocks)
        for (kind, value, start), message in zip(plan, messages):
            if kind == "group":
                links = [(i, (i + value) % groups) for i in range(groups)]
                moved[kind, value, start] = lax.ppermute(message, "tmpl", links)
            else:
                links = [(i, i ^ value) for i in range(cols)]
                moved[kind, value, start] = lax.ppermute(message, "col", links)
        return place

    firsts = sorted(range(0, cols, MEMBERS), key=lambda first: (first * 2 == cols, first))
    for first in firsts[:AHEAD]:
        place = send(first, place)

    weights = prepare_weights(
        bin_embed, row_embed, col_embed, mask_embed, layer_gain, w_in, w_out, final_gain,
        w_query, w_keyval, w_output, head_weight, head_bias,
    )
    own_codes = lax.dynamic_index_in_dim(codes, x, 0, False)
    first_messages = [moved["group", e, 0] for e in order]
    bins = jnp.stack([own_codes[:group_rows]] + [m[-2] for m in first_messages])
    tables = jnp.stack(
        [own_codes[group_rows:]] + [m[-1, : codes.shape[1] - group_rows] for m in first_messages]
    )
    tables = tables.astype(jnp.float32).reshape(groups, 2, residues)
    here = lax.dynamic_slice_in_dim(tables, z * width, width, 2)
    group_offset = x * (residues // groups) + row_offset
    there = lax.dynamic_slice_in_dim(tables, group_offset, group_rows, 2)
    masked = there[:, 0, :, None] * here[:, 0, None, :]
    bins = jnp.where(masked > 0.5, bins.astype(jnp.float32), NO_BIN)
    row_types = there[:, 1].astype(jnp.int32)
    kinds = jnp.arange(TYPE_ROWS, dtype=jnp.float32)
    col_hot = (here[:, 1, None, :] == kinds[None, :, None]).astype(jnp.bfloat16)
    own_labels = lax.dynamic_index_in_dim(label_blocks, z, 0, False)

    acc = jnp.zeros((pair_width + HEADS * HEAD_DIM + 16, head_weight.shape[1]), jnp.float32)
    loss = jnp.zeros((8, width), jnp.float32)
    for index, first in enumerate(firsts):
        members = range(first, first + MEMBERS)
        where = jnp.stack([x, z] + [z ^ d for d in members]).astype(jnp.int32)
        acc, loss, token = run_chunk(
            residues, where, row_types, act, [moved["group", e, first] for e in order],
            [moved["column", d, 0] if d else pair_act for d in members],
            [moved["column", d, 0] if d else own_labels for d in members],
            bins, col_hot, weights, acc, loss,
        )
        if index + AHEAD < len(firsts):
            send(firsts[index + AHEAD], token)

    half, classes = acc.shape[0] // 2, acc.shape[1]
    head_width = HEADS * HEAD_DIM
    bias_row = pair_width + head_width
    sums = jnp.concatenate([acc[:half], acc[half:]], axis=1)
    at_loss = (jnp.arange(half)[:, None] == bias_row + 1 - half) & (
        jnp.arange(2 * classes)[None, :] >= classes
    )
    sums = total_over_mesh(jnp.where(at_loss, jnp.sum(loss), sums))
    sums = jnp.concatenate([sums[:, :classes], sums[:, classes:]])
    head_sum = sums[:pair_width]
    bias_sum = sums[bias_row]
    output_sum = lax.dot_general(
        sums[pair_width:bias_row],
        head_weight.astype(jnp.float32),
        (((1,), (1,)), ((), ())),
        precision=lax.Precision.HIGHEST,
    )
    squares = (
        jnp.sum(head_sum * head_sum)
        + jnp.sum(bias_sum * bias_sum)
        + jnp.sum(output_sum * output_sum)
    )
    factor = CLIP_NORM / jnp.maximum(jnp.sqrt(squares), CLIP_NORM)
    return (
        sums[bias_row + 1, 0] / float(residues * residues),
        head_sum * factor,
        bias_sum * factor,
        output_sum * factor,
    )


def solution(mesh):
    in_specs = (
        P("tmpl", None, "row", None, "col"),
        P("tmpl", None, "row", "col"),
        P("tmpl", None),
        P("tmpl", None),
        P(TMPL_ROW_COL, None, None),
        P(TMPL_ROW_COL, None),
    ) + (P(),) * 13
    return jax.shard_map(
        on_device, mesh=mesh, in_specs=in_specs, out_specs=(P(),) * 4, check_vma=False
    )
```
